32 devices in a mesh: groups: 2 (over y), expert: 4 (over z), tensor: 2 (over x), sub: 2 (over core).
Axes of the slice: x: 2, y: 2, z: 4, core: 2. Of those that a mesh axis runs over, the one named last changes fastest.
Arguments:
- tokens: bfloat16 [48, 7168], P(('groups', 'expert', 'tensor'), 'sub'), parts along dimension 0, may hold values from -6 to 6
- expert_ids: int32 [48, 8], P(('groups', 'expert', 'tensor')), parts along dimension 0, may hold values from 0 to 15, all different within a row; in each aligned block of 3 rows (0 to 2, 3 to 5, ...) at most 2 rows name the same one
- gate_weights: float32 [48, 8], P(('groups', 'expert', 'tensor')), parts along dimension 0, may hold values from 0.1 to 0.6
- gate_proj: bfloat16 [16, 1024, 7168], P('expert', 'tensor', 'sub'), may hold values from -0.0625 to 0.0625
- up_proj: bfloat16 [16, 1024, 7168], P('expert', 'tensor', 'sub'), may hold values from -0.0625 to 0.0625
- down_proj: bfloat16 [16, 1024, 7168], P('expert', 'tensor', 'sub'), may hold values from -0.1875 to 0.1875
Outputs:
- blended: bfloat16 [48, 7168], P(('groups', 'expert', 'tensor'), 'sub'), parts along dimension 0
The draws below stay inside these ranges and needn't reach their ends.
There are 2 independent parts, one for each index of `groups`. The reference program is written for one: setup_inputs(seed, part) draws one part's arguments, and reference() takes and returns one part's arrays. A program takes and returns all parts, laid end to end along the dimension named above; an argument that names none is the same for every part. Nothing has to cross between parts.
Inputs may be any that keep to these rules, and one draw needn't show every extreme that they name: `expert_ids`: each row names 8 different experts. Among the rows of one owner (aligned blocks of 3 rows) no expert is named by more than 2 rows, a bound that some block reaches.
All inputs are finite; a program needn't handle non-finite values.
Results may differ from the reference program's by a relative error of at most 0.02.
Values may be sent and summed in bfloat16 or wider, within the bound.
A program may use at most 128 MiB of HBM per device.

```python
import math
import jax
import jax.numpy as jnp
import numpy as np
from jax import lax

D = 7168
TOP = 8
FW = 1024
NE = 16
TOK_DEV = 3
SLOTS = 2
TOKENS = 24
N_TENSOR = 2


def levels(own_key, dims, split, low, largest):
    loudness = 1.0
    for position, shards_of in split:
        steps = jax.random.uniform(jax.random.fold_in(jax.random.fold_in(own_key, 6), position), (shards_of,), jnp.float32, low / len(split), largest / len(split))
        loudness = loudness * jnp.repeat(jnp.exp(steps), dims[position] // shards_of).reshape((-1,) + (1,) * (len(dims) - 1 - position))
    return loudness


def routed_block(rng, own, number, rows, number_of, top, bound, lean):
    ranking = jax.random.permutation(rng, number_of)
    heavy_load, common = portions_of(number_of, rows * top, bound, lean, True), portions_of(number_of, rows * top, bound, lean, False)
    places = jnp.arange(number_of)

    def named(tallies, offset_by):
        used = int((tallies > 0).sum())
        fixed = max(1, used // 4)
        passed = fixed + (places - fixed + offset_by * (used - fixed)) % max(1, number_of - fixed)
        return jnp.zeros((number_of,), jnp.int32).at[ranking[jnp.where(places < fixed, places, passed)]].set(jnp.asarray(tallies, jnp.int32))

    tallies = jnp.where(number % 4 == 0, named(heavy_load, number // 4), named(common, number - number // 4 - 1))
    mixed = jax.random.permutation(jax.random.fold_in(own, 3), number_of)
    donor, receiver = mixed[0:number_of // 2 * 2:2], mixed[1:number_of // 2 * 2:2]
    slack = jnp.minimum(tallies[donor] - 1, bound - tallies[receiver]) // 2
    slack = jnp.where((donor == ranking[0]) | (receiver == ranking[0]) | (tallies[receiver] == 0), 0, jnp.maximum(slack, 0))
    passed = jax.random.randint(jax.random.fold_in(own, 4), (number_of // 2,), 0, 1 << 20) % (slack + 1)
    tallies = tallies.at[donor].add(-passed).at[receiver].add(passed)
    items = jnp.searchsorted(jnp.cumsum(tallies), jnp.arange(rows * top), side="right").astype(jnp.int32)
    listing = items.reshape(top, rows).T
    listing = listing[jax.random.permutation(jax.random.fold_in(own, 1), rows)]
    offset_by = jax.random.randint(jax.random.fold_in(own, 2), (rows, 1), 0, top)
    return jnp.take_along_axis(listing, (jnp.arange(top)[None, :] + offset_by) % top, axis=1)


def portions_of(count, total, reach, skew, full):
    loads = [(1 << 20) // math.isqrt(rank ** skew) + 1 for rank in range(1, count + 1)]
    largest = reach if full else min(reach, max(-(-total // count), total * loads[0] // sum(loads)))
    least = 1 if total - largest >= count - 1 else 0
    holding, spare = [largest] + [least] * (count - 1), total - largest - least * (count - 1)
    while spare > 0:
        free = [i for i in range(1, count) if holding[i] < largest] or [i for i in range(1, count) if holding[i] < reach]
        mass, remaining = sum([loads[i] for i in free]), spare
        for i in free:
            extra = min(reach - holding[i], max(1, remaining * loads[i] // mass), spare)
            holding[i] = holding[i] + extra
            spare = spare - extra
    return np.array(holding)


def gaussian(stream_key, dims, scale, most, shards=(), held_as=jnp.bfloat16):
    drawn = scale * jax.random.normal(stream_key, dims, jnp.float32)
    if shards:
        drawn = drawn * levels(stream_key, dims, shards, -0.22, 0.18)
    return jnp.clip(drawn, -most, most).astype(held_as)


def setup_inputs(seed: int = 0, part: int = 0) -> dict:
    seeds = jax.random.split(jax.random.key(seed), 7)
    part_keys = jax.random.split(jax.random.fold_in(seeds[6], part), 7)
    tokens = gaussian(part_keys[0], (TOKENS, D), 1.0, 6.0, ((0, 8), (1, 2)))
    expert_ids_keys = jax.random.split(jax.random.fold_in(part_keys[1], 1), TOKENS // TOK_DEV)
    expert_ids_turns = jax.random.permutation(jax.random.fold_in(part_keys[1], 3), TOKENS // TOK_DEV)
    expert_ids = jax.vmap(lambda own, number: routed_block(jax.random.fold_in(part_keys[1], 2), own, number, TOK_DEV, NE, TOP, SLOTS, 2))(expert_ids_keys, expert_ids_turns).reshape((TOKENS, TOP))
    gate_weights = jnp.clip(0.1 + 0.5 * jax.random.uniform(part_keys[2], (TOKENS, TOP), jnp.float32) ** levels(part_keys[2], (TOKENS, TOP), ((0, 8),), -0.2, 0.2), 0.1, 0.6)
    gate_proj = gaussian(seeds[3], (NE, FW, D), D ** -0.5, 0.0625, ((0, 4), (1, 2), (2, 2)))
    up_proj = gaussian(seeds[4], (NE, FW, D), D ** -0.5, 0.0625, ((0, 4), (1, 2), (2, 2)))
    down_proj = gaussian(seeds[5], (NE, FW, D), FW ** -0.5, 0.1875, ((0, 4), (1, 2), (2, 2)))
    return {"tokens": tokens, "expert_ids": expert_ids, "gate_weights": gate_weights, "gate_proj": gate_proj, "up_proj": up_proj, "down_proj": down_proj}


def reference(tokens, expert_ids, gate_weights, gate_proj, up_proj, down_proj):
    count = tokens.shape[0]
    block = FW // N_TENSOR
    labels = jnp.arange(NE, dtype=jnp.int32)
    chosen = (expert_ids[:, :, None] == labels[None, None, :]).astype(jnp.float32)
    weight_table = jnp.sum(gate_weights[:, :, None].astype(jnp.float32) * chosen, axis=1)
    inputs_wide = tokens.astype(jnp.float32)

    def one_expert(total, inputs):
        gate_rows, up_rows, down_rows, weight_column = inputs
        gate = lax.dot_general(inputs_wide, gate_rows.astype(jnp.float32), (((1,), (1,)), ((), ())), precision=lax.Precision.HIGHEST)
        upper = lax.dot_general(inputs_wide, up_rows.astype(jnp.float32), (((1,), (1,)), ((), ())), precision=lax.Precision.HIGHEST)
        hidden = (jax.nn.silu(gate) * upper).astype(jnp.bfloat16)
        pieces = jnp.einsum("ntf,tfd->ntd", hidden.reshape(count, N_TENSOR, block).astype(jnp.float32), down_rows.reshape(N_TENSOR, block, D).astype(jnp.float32), precision=lax.Precision.HIGHEST)
        pieces = lax.optimization_barrier(pieces.astype(jnp.bfloat16)).astype(jnp.float32)
        expert_out = jnp.sum(pieces, axis=1)
        return total + weight_column[:, None] * expert_out, None

    start = jnp.zeros((count, D), jnp.float32)
    total, unused = lax.scan(one_expert, start, (gate_proj, up_proj, down_proj, weight_table.T))
    return total.astype(jnp.bfloat16)
```

```python
import functools

import jax
import jax.numpy as jnp
from jax import lax
from jax.experimental import pallas as pl
from jax.experimental.pallas import tpu as pltpu
from jax.sharding import PartitionSpec as P

MESH = pl.DeviceIdType.MESH
PIECES = 2
EARLY = 2
NT = (((1,), (1,)), ((), ()))


def kernel(
    sizes,
    tok_ref, ids_ref, gw_ref, gate_ref, up_ref, down_ref, out_ref,
    wg, wu, wd, tok_in, ids_in, gw_in, x32, x16, ids_all, gw_all,
    own_part, sent_part, got_part, hidden, y, stage, ret,
    w_sem, in_send, in_recv, part_send, part_recv, ret_send, ret_recv,
):
    expert_count, tensor_count, sub_count = sizes
    peers = expert_count * tensor_count
    local_count, units = gate_ref.shape[0], gate_ref.shape[1]
    owned, features = tok_ref.shape
    width = features // PIECES
    expert_at = lax.axis_index("expert")
    me = expert_at * tensor_count + lax.axis_index("tensor")
    sub = lax.axis_index("sub")

    def peer(k):
        p = lax.rem(me + k, peers)
        return p, {"expert": p // tensor_count, "tensor": lax.rem(p, tensor_count)}

    def core(j):
        return {"sub": lax.rem(sub + j, sub_count)}

    barrier = pltpu.get_barrier_semaphore()

    def greet(k, carry):
        pl.semaphore_signal(barrier, inc=1, device_id=peer(k)[1], device_id_type=MESH)
        return carry

    lax.fori_loop(1, peers, greet, 0)
    for j in range(1, sub_count):
        pl.semaphore_signal(barrier, inc=1, device_id=core(j), device_id_type=MESH)

    loads = []
    for l in range(local_count):
        loads.append(pltpu.make_async_copy(gate_ref.at[l], wg.at[l], w_sem.at[0, l]))
        loads.append(pltpu.make_async_copy(up_ref.at[l], wu.at[l], w_sem.at[1, l]))
    for l in range(local_count):
        loads.append(pltpu.make_async_copy(down_ref.at[l], wd.at[l], w_sem.at[2, l]))
    inputs = ((tok_ref, tok_in), (ids_ref, ids_in), (gw_ref, gw_in))
    for i, (src, dst) in enumerate(inputs):
        pltpu.make_async_copy(src, dst.at[me], in_recv.at[i]).start()
    early = 2 * min(EARLY, local_count)
    for load in loads[:early]:
        load.start()

    pl.semaphore_wait(barrier, peers - 1 + sub_count - 1)

    def dispatch(k, carry):
        _, where = peer(k)
        for i, (src, dst) in enumerate(inputs):
            pltpu.make_async_remote_copy(
                src_ref=src, dst_ref=dst.at[me], send_sem=in_send.at[i], recv_sem=in_recv.at[i],
                device_id=where, device_id_type=MESH,
            ).start()
        return carry

    lax.fori_loop(1, peers, dispatch, 0)
    for load in loads[early:]:
        load.start()

    for i, (_, dst) in enumerate(inputs):
        pltpu.make_async_copy(dst, dst, in_recv.at[i]).wait()
    for p in range(peers):
        rows = pl.ds(p * owned, owned)
        x32[rows, :] = tok_in[p].astype(jnp.float32)
        ids_all[rows, :] = ids_in[p]
        gw_all[rows, :] = gw_in[p]
    x16[...] = x32[...].astype(jnp.bfloat16)

    def first(l):
        x = x16[...]
        loads[2 * l].wait()
        gate = lax.dot_general(x, wg[l], NT, preferred_element_type=jnp.float32)
        own_part[l, :, :units] = gate
        sent_part[l, :, :units] = gate.astype(jnp.bfloat16)
        loads[2 * l + 1].wait()
        up = lax.dot_general(x, wu[l], NT, preferred_element_type=jnp.float32)
        own_part[l, :, units:] = up
        sent_part[l, :, units:] = up.astype(jnp.bfloat16)
        for j in range(1, sub_count):
            exchange(l, j).start()

    def exchange(l, j):
        return pltpu.make_async_remote_copy(
            src_ref=sent_part.at[l], dst_ref=got_part.at[l, j - 1],
            send_sem=part_send.at[l, j - 1], recv_sem=part_recv.at[l, j - 1],
            device_id=core(j), device_id_type=MESH,
        )

    def finish(l):
        both = own_part[l]
        for j in range(1, sub_count):
            exchange(l, j).wait()
            both = both + got_part[l, j - 1].astype(jnp.float32)
        gate, up = both[:, :units], both[:, units:]
        label = expert_at * local_count + l
        weight = jnp.sum(jnp.where(ids_all[...] == label, gw_all[...], 0.0), axis=1, keepdims=True)
        hidden[l] = (gate / (1.0 + jnp.exp(-gate)) * up * weight).astype(jnp.bfloat16)

    for l in range(local_count):
        first(l)
        if l > 0:
            finish(l - 1)
    last = local_count - 1
    for l in range(last):
        loads[2 * local_count + l].wait()
        part = jnp.dot(hidden[l], wd[l], preferred_element_type=jnp.float32)
        y[...] = part if l == 0 else y[...] + part
    finish(last)
    loads[2 * local_count + last].wait()

    for c in range(PIECES):
        columns = pl.ds(c * width, width)
        part = jnp.dot(hidden[last], wd[last, :, columns], preferred_element_type=jnp.float32)
        if last > 0:
            part = part + y[:, columns]
        for p in range(peers):
            stage[c, p] = part[p * owned:(p + 1) * owned].astype(jnp.bfloat16)

        def give(k, carry):
            p, where = peer(k)
            pltpu.make_async_remote_copy(
                src_ref=stage.at[c, p], dst_ref=ret.at[c, me], send_sem=ret_send.at[c],
                recv_sem=ret_recv.at[c], device_id=where, device_id_type=MESH,
            ).start()
            return carry

        lax.fori_loop(1, peers, give, 0)

    for c in range(PIECES):
        columns = pl.ds(c * width, width)
        some = ret.at[c, pl.ds(0, peers - 1)]
        pltpu.make_async_copy(some, some, ret_recv.at[c]).wait()
        total = stage[c, me].astype(jnp.float32)
        for k in range(1, peers):
            total = total + ret[c, peer(k)[0]].astype(jnp.float32)
        out_ref[:, columns] = total.astype(jnp.bfloat16)

    for i, (_, dst) in enumerate(inputs):
        some = dst.at[pl.ds(0, peers - 1)]
        pltpu.make_async_copy(some, some, in_send.at[i]).wait()
    for c in range(PIECES):
        some = ret.at[c, pl.ds(0, peers - 1)]
        pltpu.make_async_copy(some, some, ret_send.at[c]).wait()


def solution(mesh):
    expert_count, tensor_count = mesh.shape["expert"], mesh.shape["tensor"]
    sub_count = mesh.shape["sub"]
    peers = expert_count * tensor_count

    def per_device(tokens, expert_ids, gate_weights, gate_proj, up_proj, down_proj):
        owned, features = tokens.shape
        top = expert_ids.shape[1]
        local_count, units = gate_proj.shape[0], gate_proj.shape[1]
        rows = peers * owned
        others = max(1, sub_count - 1)
        width = features // PIECES
        bf16, f32 = jnp.bfloat16, jnp.float32
        dma = pltpu.SemaphoreType.DMA
        hbm = pl.BlockSpec(memory_space=pl.ANY)
        return pl.pallas_call(
            functools.partial(kernel, (expert_count, tensor_count, sub_count)),
            out_shape=jax.ShapeDtypeStruct((owned, features), bf16),
            in_specs=[hbm] * 6,
            out_specs=pl.BlockSpec(memory_space=pltpu.VMEM),
            scratch_shapes=[
                pltpu.VMEM(gate_proj.shape, bf16),
                pltpu.VMEM(up_proj.shape, bf16),
                pltpu.VMEM(down_proj.shape, bf16),
                pltpu.VMEM((peers, owned, features), bf16),
                pltpu.VMEM((peers, owned, top), jnp.int32),
                pltpu.VMEM((peers, owned, top), f32),
                pltpu.VMEM((rows, features), f32),
                pltpu.VMEM((rows, features), bf16),
                pltpu.VMEM((rows, top), jnp.int32),
                pltpu.VMEM((rows, top), f32),
                pltpu.VMEM((local_count, rows, 2 * units), f32),
                pltpu.VMEM((local_count, rows, 2 * units), bf16),
                pltpu.VMEM((local_count, others, rows, 2 * units), bf16),
                pltpu.VMEM((local_count, rows, units), bf16),
                pltpu.VMEM((rows, features), f32),
                pltpu.VMEM((PIECES, peers, owned, width), bf16),
                pltpu.VMEM((PIECES, peers, owned, width), bf16),
                dma((3, local_count)),
                dma((3,)),
                dma((3,)),
                dma((local_count, others)),
                dma((local_count, others)),
                dma((PIECES,)),
                dma((PIECES,)),
            ],
            compiler_params=pltpu.CompilerParams(
                collective_id=0, has_side_effects=True, vmem_limit_bytes=60 * 1024 * 1024
            ),
        )(tokens, expert_ids, gate_weights, gate_proj, up_proj, down_proj)

    placed = (
        P(("groups", "expert", "tensor"), "sub"),
        P(("groups", "expert", "tensor"), None),
        P(("groups", "expert", "tensor"), None),
        P("expert", "tensor", "sub"),
        P("expert", "tensor", "sub"),
        P("expert", "tensor", "sub"),
    )
    return jax.shard_map(
        per_device,
        mesh=mesh,
        in_specs=placed,
        out_specs=P(("groups", "expert", "tensor"), "sub"),
        check_vma=False,
    )
```

```python
import functools

import jax
import jax.numpy as jnp
from jax import lax
from jax.experimental import pallas as pl
from jax.experimental.pallas import tpu as pltpu
from jax.sharding import PartitionSpec as P

MESH = pl.DeviceIdType.MESH
PIECES = 1
TURNED = 2
EARLY = 2
NT = (((1,), (1,)), ((), ()))


def kernel(
    sizes,
    tok_ref, ids_ref, gw_ref, gate_ref, up_ref, down_ref, out_ref,
    wg, wu, wd, tok_in, ids_in, gw_in, x32, x16, ids_all, gw_all,
    own_part, sent_part, got_part, hidden, y, stage, ret,
    turned, w_sem, in_send, in_recv, part_send, part_recv, ret_send, ret_recv,
):
    expert_count, tensor_count, sub_count = sizes
    peers = expert_count * tensor_count
    local_count, units = gate_ref.shape[0], gate_ref.shape[1]
    owned, features = tok_ref.shape
    width = features // PIECES
    expert_at = lax.axis_index("expert")
    me = expert_at * tensor_count + lax.axis_index("tensor")
    sub = lax.axis_index("sub")

    def peer(k):
        p = lax.rem(me + k, peers)
        return p, {"expert": p // tensor_count, "tensor": lax.rem(p, tensor_count)}

    def core(j):
        return {"sub": lax.rem(sub + j, sub_count)}

    barrier = pltpu.get_barrier_semaphore()

    def greet(k, carry):
        pl.semaphore_signal(barrier, inc=1, device_id=peer(k)[1], device_id_type=MESH)
        return carry

    lax.fori_loop(1, peers, greet, 0, unroll=peers <= 16)
    for j in range(1, sub_count):
        pl.semaphore_signal(barrier, inc=1, device_id=core(j), device_id_type=MESH)

    loads = []
    for l in range(local_count):
        loads.append(pltpu.make_async_copy(gate_ref.at[l], wg.at[l], w_sem.at[0, l]))
        loads.append(pltpu.make_async_copy(up_ref.at[l], wu.at[l], w_sem.at[1, l]))
    for l in range(local_count):
        loads.append(pltpu.make_async_copy(down_ref.at[l], wd.at[l], w_sem.at[2, l]))
    inputs = ((tok_ref, tok_in), (ids_ref, ids_in), (gw_ref, gw_in))
    for i, (src, dst) in enumerate(inputs):
        pltpu.make_async_copy(src, dst.at[me], in_recv.at[i]).start()
    early = 2 * min(EARLY, local_count)
    for load in loads[:early]:
        load.start()

    pl.semaphore_wait(barrier, peers - 1 + sub_count - 1)

    def dispatch(k, carry):
        _, where = peer(k)
        for i, (src, dst) in enumerate(inputs):
            pltpu.make_async_remote_copy(
                src_ref=src, dst_ref=dst.at[me], send_sem=in_send.at[i], recv_sem=in_recv.at[i],
                device_id=where, device_id_type=MESH,
            ).start()
        return carry

    lax.fori_loop(1, peers, dispatch, 0, unroll=peers <= 16)
    for load in loads[early:]:
        load.start()

    stage[...] = jnp.zeros_like(stage)
    for l in range(min(TURNED, local_count)):
        loads[2 * l].wait()
        turned[2 * l] = wg[l].T
        loads[2 * l + 1].wait()
        turned[2 * l + 1] = wu[l].T
    for i, (_, dst) in enumerate(inputs):
        pltpu.make_async_copy(dst, dst, in_recv.at[i]).wait()
    for p in range(peers):
        rows = pl.ds(p * owned, owned)
        x32[rows, :] = tok_in[p].astype(jnp.float32)
        ids_all[rows, :] = ids_in[p]
        gw_all[rows, :] = gw_in[p]
    x16[...] = x32[...].astype(jnp.bfloat16)

    def first(l):
        x = x16[...]
        if l < TURNED:
            gate = jnp.dot(x, turned[2 * l], preferred_element_type=jnp.float32)
            up = jnp.dot(x, turned[2 * l + 1], preferred_element_type=jnp.float32)
            own_part[l, :, :units] = gate
            sent_part[l, :, :units] = gate.astype(jnp.bfloat16)
            own_part[l, :, units:] = up
            sent_part[l, :, units:] = up.astype(jnp.bfloat16)
            for j in range(1, sub_count):
                exchange(l, j).start()
            return
        loads[2 * l].wait()
        gate = lax.dot_general(x, wg[l], NT, preferred_element_type=jnp.float32)
        own_part[l, :, :units] = gate
        sent_part[l, :, :units] = gate.astype(jnp.bfloat16)
        loads[2 * l + 1].wait()
        up = lax.dot_general(x, wu[l], NT, preferred_element_type=jnp.float32)
        own_part[l, :, units:] = up
        sent_part[l, :, units:] = up.astype(jnp.bfloat16)
        for j in range(1, sub_count):
            exchange(l, j).start()

    def exchange(l, j):
        return pltpu.make_async_remote_copy(
            src_ref=sent_part.at[l], dst_ref=got_part.at[l, j - 1],
            send_sem=part_send.at[l, j - 1], recv_sem=part_recv.at[l, j - 1],
            device_id=core(j), device_id_type=MESH,
        )

    def finish(l):
        both = own_part[l]
        for j in range(1, sub_count):
            exchange(l, j).wait()
            both = both + got_part[l, j - 1].astype(jnp.float32)
        gate, up = both[:, :units], both[:, units:]
        label = expert_at * local_count + l
        weight = jnp.sum(jnp.where(ids_all[...] == label, gw_all[...], 0.0), axis=1, keepdims=True)
        hidden[l] = (gate / (1.0 + jnp.exp(-gate)) * up * weight).astype(jnp.bfloat16)

    for l in range(local_count):
        first(l)
        if l > 0:
            finish(l - 1)
    last = local_count - 1
    for l in range(last):
        loads[2 * local_count + l].wait()
        part = jnp.dot(hidden[l], wd[l], preferred_element_type=jnp.float32)
        y[...] = part if l == 0 else y[...] + part
    finish(last)
    loads[2 * local_count + last].wait()

    for c in range(PIECES):
        columns = pl.ds(c * width, width)
        part = jnp.dot(hidden[last], wd[last, :, columns], preferred_element_type=jnp.float32)
        if last > 0:
            part = part + y[:, columns]
        for p in range(peers):
            stage[c, p, :owned] = part[p * owned:(p + 1) * owned].astype(jnp.bfloat16)

        def give(k, carry):
            p, where = peer(k)
            pltpu.make_async_remote_copy(
                src_ref=stage.at[c, p], dst_ref=ret.at[c, me], send_sem=ret_send.at[c],
                recv_sem=ret_recv.at[c], device_id=where, device_id_type=MESH,
            ).start()
            return carry

        lax.fori_loop(1, peers, give, 0, unroll=peers <= 16)

    for c in range(PIECES):
        columns = pl.ds(c * width, width)
        some = ret.at[c, pl.ds(0, peers - 1)]
        pltpu.make_async_copy(some, some, ret_recv.at[c]).wait()
        total = stage[c, me, :owned].astype(jnp.float32)
        for k in range(1, peers):
            total = total + ret[c, peer(k)[0], :owned].astype(jnp.float32)
        out_ref[:, columns] = total.astype(jnp.bfloat16)

    for i, (_, dst) in enumerate(inputs):
        some = dst.at[pl.ds(0, peers - 1)]
        pltpu.make_async_copy(some, some, in_send.at[i]).wait()
    for c in range(PIECES):
        some = ret.at[c, pl.ds(0, peers - 1)]
        pltpu.make_async_copy(some, some, ret_send.at[c]).wait()


def solution(mesh):
    expert_count, tensor_count = mesh.shape["expert"], mesh.shape["tensor"]
    sub_count = mesh.shape["sub"]
    peers = expert_count * tensor_count

    def per_device(tokens, expert_ids, gate_weights, gate_proj, up_proj, down_proj):
        owned, features = tokens.shape
        top = expert_ids.shape[1]
        local_count, units = gate_proj.shape[0], gate_proj.shape[1]
        rows = peers * owned
        others = max(1, sub_count - 1)
        width = features // PIECES
        padded = pl.cdiv(owned, 4) * 4
        bf16, f32 = jnp.bfloat16, jnp.float32
        dma = pltpu.SemaphoreType.DMA
        hbm = pl.BlockSpec(memory_space=pl.ANY)
        return pl.pallas_call(
            functools.partial(kernel, (expert_count, tensor_count, sub_count)),
            out_shape=jax.ShapeDtypeStruct((owned, features), bf16),
            in_specs=[hbm] * 6,
            out_specs=pl.BlockSpec(memory_space=pltpu.VMEM),
            scratch_shapes=[
                pltpu.VMEM(gate_proj.shape, bf16),
                pltpu.VMEM(up_proj.shape, bf16),
                pltpu.VMEM(down_proj.shape, bf16),
                pltpu.VMEM((peers, owned, features), bf16),
                pltpu.VMEM((peers, owned, top), jnp.int32),
                pltpu.VMEM((peers, owned, top), f32),
                pltpu.VMEM((rows, features), f32),
                pltpu.VMEM((rows, features), bf16),
                pltpu.VMEM((rows, top), jnp.int32),
                pltpu.VMEM((rows, top), f32),
                pltpu.VMEM((local_count, rows, 2 * units), f32),
                pltpu.VMEM((local_count, rows, 2 * units), bf16),
                pltpu.VMEM((local_count, others, rows, 2 * units), bf16),
                pltpu.VMEM((local_count, rows, units), bf16),
                pltpu.VMEM((rows, features), f32),
                pltpu.VMEM((PIECES, peers, padded, width), bf16),
                pltpu.VMEM((PIECES, peers, padded, width), bf16),
                pltpu.VMEM((2 * min(TURNED, local_count), features, units), bf16),
                dma((3, local_count)),
                dma((3,)),
                dma((3,)),
                dma((local_count, others)),
                dma((local_count, others)),
                dma((PIECES,)),
                dma((PIECES,)),
            ],
            compiler_params=pltpu.CompilerParams(
                collective_id=0, has_side_effects=True, vmem_limit_bytes=60 * 1024 * 1024
            ),
        )(tokens, expert_ids, gate_weights, gate_proj, up_proj, down_proj)

    placed = (
        P(("groups", "expert", "tensor"), "sub"),
        P(("groups", "expert", "tensor"), None),
        P(("groups", "expert", "tensor"), None),
        P("expert", "tensor", "sub"),
        P("expert", "tensor", "sub"),
        P("expert", "tensor", "sub"),
    )
    return jax.shard_map(
        per_device,
        mesh=mesh,
        in_specs=placed,
        out_specs=P(("groups", "expert", "tensor"), "sub"),
        check_vma=False,
    )
```
